256 devices in a mesh: dp: 32 (over x, z), section: 8 (over y, core).
Axes of the slice: x: 4, y: 4, z: 8, core: 2. Of those that a mesh axis runs over, the one named last changes fastest.
Arguments:
- hidden_in: bfloat16 [8, 4, 32, 96, 2048], P('section', None, 'dp'), may hold values from -170 to 170
- queries: bfloat16 [8, 4, 32, 96, 2048], P('section', None, 'dp'), may hold values from -96 to 96
- keys: bfloat16 [8, 4, 32, 96, 2048], P('section', None, 'dp'), may hold values from -6 to 6
- values: bfloat16 [8, 4, 32, 96, 2048], P('section', None, 'dp'), may hold values from -6 to 6
- cotangent: bfloat16 [4, 32, 96, 2048], P(None, 'dp'), may hold values from -6 to 6
- norm_gain: float32 [8, 2048], P('section'), may hold values from 0.1 to 1.9
- w_query: bfloat16 [8, 2048, 2048], P('section', 'dp'), may hold values from -0.125 to 0.125
- w_key: bfloat16 [8, 2048, 2048], P('section', 'dp'), may hold values from -0.125 to 0.125
- w_value: bfloat16 [8, 2048, 2048], P('section', 'dp'), may hold values from -0.125 to 0.125
- down_q: bfloat16 [8, 16, 2048], P('section'), may hold values from -0.125 to 0.125
- up_q: bfloat16 [8, 16, 2048], P('section'), may hold values from -0.75 to 0.75
- down_v: bfloat16 [8, 16, 2048], P('section'), may hold values from -0.125 to 0.125
- up_v: bfloat16 [8, 16, 2048], P('section'), may hold values from -0.75 to 0.75
Outputs:
- input_grad: bfloat16 [8, 4, 32, 96, 2048], P('section', None, 'dp')
- grad_down_q: float32 [8, 16, 2048], P('section')
- grad_up_q: float32 [8, 16, 2048], P('section')
- grad_down_v: float32 [8, 16, 2048], P('section')
- grad_up_v: float32 [8, 16, 2048], P('section')
The draws below stay inside these ranges and needn't reach their ends.
All inputs are finite; a program needn't handle non-finite values.
Results may differ from the reference program's by a relative error of at most 0.025.
Values may be sent and summed in bfloat16 or wider, within the bound.
No kernel may reach another device: no remote copies, remote signals or barrier semaphores. Data moves between devices by JAX's collectives and lax.ppermute only.
A program may use at most 128 MiB of HBM per device.

```python
import jax
import jax.numpy as jnp
from jax import lax

HEADS = 16
HEAD_DIM = 128
D = 2048
RANK = 16
MICRO = 4
SEQ = 96
LAYERS = 8
BATCH = 32


def attention_pair(key):
    full_shape = (LAYERS, MICRO, BATCH, SEQ, HEADS, HEAD_DIM)
    first = jax.random.normal(jax.random.fold_in(key, 11), full_shape, jnp.float32)
    second = jax.random.normal(jax.random.fold_in(key, 23), full_shape, jnp.float32)
    query = jnp.clip(first, -6.0, 6.0)
    keyed = jnp.clip(second, -6.0, 6.0)
    final_shape = (LAYERS, MICRO, BATCH, SEQ, HEADS * HEAD_DIM)
    return (query.reshape(final_shape), keyed.reshape(final_shape))


def draw_queries(key, part):
    return attention_pair(key)[0].astype(jnp.bfloat16)


def draw_keys(key, part):
    return attention_pair(key)[1].astype(jnp.bfloat16)


def draw_hidden_in(key, part):
    full_shape = (LAYERS, MICRO, BATCH, SEQ, D)
    base = jnp.clip(jax.random.normal(jax.random.fold_in(key, 41), full_shape, jnp.float32), -6.0, 6.0)
    return base.astype(jnp.bfloat16)


def level_of(stream_key, dims, shards, low, high):
    gain, own = 1.0, jax.random.fold_in(stream_key, 6)
    for axis_at, blocks in shards:
        steps = jnp.exp(jax.random.uniform(jax.random.fold_in(own, axis_at), (blocks,), jnp.float32, low / len(shards), high / len(shards)))
        gain = gain * jnp.repeat(steps, dims[axis_at] // blocks).reshape([-1 if axis == axis_at else 1 for axis in range(len(dims))])
    return gain


def normal_values(rng, shape, deviation, bound, cuts=(), kind=jnp.bfloat16):
    gain = level_of(rng, shape, cuts, -0.22, 0.18) if cuts else 1.0
    drawn = jax.random.normal(rng, shape, jnp.float32) * deviation * gain
    return jnp.minimum(jnp.maximum(drawn, -bound), bound).astype(kind)


def setup_inputs(seed: int = 0) -> dict:
    splits = jax.random.split(jax.random.key(seed), 14)
    hidden_in = draw_hidden_in(jax.random.fold_in(splits[13], 71), 0)
    queries = draw_queries(jax.random.fold_in(splits[13], 71), 0)
    keys = draw_keys(jax.random.fold_in(splits[13], 71), 0)
    values = normal_values(splits[3], (LAYERS, MICRO, BATCH, SEQ, D), 1.0, 6.0, ((0, 8), (2, 32)))
    cotangent = normal_values(splits[4], (MICRO, BATCH, SEQ, D), 1.0, 6.0, ((1, 32),))
    norm_gain = jnp.clip(1.0 + 0.18 * jax.random.normal(splits[5], (LAYERS, D), jnp.float32), 0.1, 1.9)
    w_query = normal_values(splits[6], (LAYERS, D, D), D ** -0.5, 0.125, ((0, 8), (1, 32)))
    w_key = normal_values(splits[7], (LAYERS, D, D), D ** -0.5, 0.125, ((0, 8), (1, 32)))
    w_value = normal_values(splits[8], (LAYERS, D, D), D ** -0.5, 0.125, ((0, 8), (1, 32)))
    down_q = normal_values(splits[9], (LAYERS, RANK, D), D ** -0.5, 0.125, ((0, 8),))
    up_q = normal_values(splits[10], (LAYERS, RANK, D), (4 * RANK) ** -0.5, 0.75, ((0, 8),))
    down_v = normal_values(splits[11], (LAYERS, RANK, D), D ** -0.5, 0.125, ((0, 8),))
    up_v = normal_values(splits[12], (LAYERS, RANK, D), (4 * RANK) ** -0.5, 0.75, ((0, 8),))
    return {"hidden_in": hidden_in, "queries": queries, "keys": keys, "values": values, "cotangent": cotangent, "norm_gain": norm_gain, "w_query": w_query, "w_key": w_key, "w_value": w_value, "down_q": down_q, "up_q": up_q, "down_v": down_v, "up_v": up_v}


adapter_scale = 2.0
norm_eps = 1e-05

def input_backward(hidden, query, keyed, valued, out_grad, gain_row, frozen, adapter_weights):
    count, positions, features = hidden.shape
    head_count = features // HEAD_DIM
    scale = HEAD_DIM ** (-0.5)
    floated = hidden.astype(jnp.float32)
    inverse = lax.rsqrt(lax.optimization_barrier(jnp.mean(floated * floated, axis=-1, keepdims=True)) + norm_eps)
    normed = (floated * inverse * gain_row).astype(jnp.bfloat16)
    split = (count, positions, head_count, HEAD_DIM)
    query_heads = query.astype(jnp.float32).reshape(split)
    key_heads = keyed.astype(jnp.float32).reshape(split)
    value_heads = valued.astype(jnp.float32).reshape(split)
    grad_heads = out_grad.astype(jnp.float32).reshape(split)
    scores = jnp.einsum('nqhd,nkhd->nhqk', query_heads, key_heads) * scale
    causal = lax.broadcasted_iota(jnp.int32, (positions, positions), 1) <= lax.broadcasted_iota(jnp.int32, (positions, positions), 0)
    scores = jnp.where(causal, scores, -1e+30)
    attend = jax.nn.softmax(scores, axis=-1)
    attend_low = lax.optimization_barrier(attend.astype(jnp.bfloat16)).astype(jnp.float32)
    attend_grad = jnp.einsum('nqhd,nkhd->nhqk', grad_heads, value_heads)
    value_grad = jnp.einsum('nhqk,nqhd->nkhd', attend_low, grad_heads).astype(jnp.bfloat16)
    row_total = lax.optimization_barrier(jnp.sum(attend * attend_grad, axis=-1, keepdims=True))
    score_grad = (attend * (attend_grad - row_total) * scale).astype(jnp.bfloat16)
    score_wide = lax.optimization_barrier(score_grad).astype(jnp.float32)
    query_grad = jnp.einsum('nhqk,nkhd->nqhd', score_wide, key_heads).astype(jnp.bfloat16)
    key_grad = jnp.einsum('nhqk,nqhd->nkhd', score_wide, query_heads).astype(jnp.bfloat16)
    rows = count * positions
    flattened_query = query_grad.reshape(rows, features)
    key_flat = key_grad.reshape(rows, features)
    flattened_value = value_grad.reshape(rows, features)
    contract_matrices = (((1,), (1,)), ((), ()))
    normed_grad = lax.dot_general(flattened_query, frozen[0], contract_matrices, preferred_element_type=jnp.float32)
    normed_grad = normed_grad + lax.dot_general(key_flat, frozen[1], contract_matrices, preferred_element_type=jnp.float32)
    normed_grad = normed_grad + lax.dot_general(flattened_value, frozen[2], contract_matrices, preferred_element_type=jnp.float32)
    query_low_rank = (adapter_scale * lax.dot_general(flattened_query, adapter_weights[1], contract_matrices, preferred_element_type=jnp.float32)).astype(jnp.bfloat16)
    value_low_rank = (adapter_scale * lax.dot_general(flattened_value, adapter_weights[3], contract_matrices, preferred_element_type=jnp.float32)).astype(jnp.bfloat16)
    normed_grad = normed_grad + jnp.dot(query_low_rank, adapter_weights[0], preferred_element_type=jnp.float32)
    normed_grad = normed_grad + jnp.dot(value_low_rank, adapter_weights[2], preferred_element_type=jnp.float32)
    scaled_grad = (gain_row * normed_grad).reshape(count, positions, features)
    correction = lax.optimization_barrier(jnp.mean(floated * scaled_grad, axis=-1, keepdims=True))
    input_grad = (out_grad.astype(jnp.float32) + inverse * scaled_grad - floated * inverse ** 3 * correction).astype(jnp.bfloat16)
    saved = (normed.reshape(rows, features), flattened_query, flattened_value, query_low_rank, value_low_rank)
    return (input_grad, saved)

def adapter_grads(normed, flattened_query, flattened_value, query_low_rank, value_low_rank, down_query, down_value):
    contract_matrices = (((1,), (1,)), ((), ()))
    across_replicas_total = (((0,), (0,)), ((), ()))
    normalized_query = lax.dot_general(normed, down_query, contract_matrices, preferred_element_type=jnp.float32).astype(jnp.bfloat16)
    normalized_value = lax.dot_general(normed, down_value, contract_matrices, preferred_element_type=jnp.float32).astype(jnp.bfloat16)
    grad_dq = lax.dot_general(query_low_rank, normed, across_replicas_total, preferred_element_type=jnp.float32)
    query_up_gradient = adapter_scale * lax.dot_general(normalized_query, flattened_query, across_replicas_total, preferred_element_type=jnp.float32)
    grad_dv = lax.dot_general(value_low_rank, normed, across_replicas_total, preferred_element_type=jnp.float32)
    value_up_gradient = adapter_scale * lax.dot_general(normalized_value, flattened_value, across_replicas_total, preferred_element_type=jnp.float32)
    return (grad_dq, query_up_gradient, grad_dv, value_up_gradient)

def reference(hidden_in, queries, keys, values, cotangent, norm_gain, w_query, w_key, w_value, down_q, up_q, down_v, up_v):
    count = MICRO * BATCH
    out_grad = cotangent.reshape(count, SEQ, D)
    input_list = []
    grad_lists = ([], [], [], [])
    for current in reversed(range(LAYERS)):
        frozen = (w_query[current], w_key[current], w_value[current])
        adapter_weights = (down_q[current], up_q[current], down_v[current], up_v[current])
        input_grad, saved = input_backward(hidden_in[current].reshape(count, SEQ, D), queries[current].reshape(count, SEQ, D), keys[current].reshape(count, SEQ, D), values[current].reshape(count, SEQ, D), out_grad, norm_gain[current], frozen, adapter_weights)
        totals = adapter_grads(*saved, adapter_weights[0], adapter_weights[2])
        input_list.append(input_grad)
        for target, total in zip(grad_lists, totals):
            target.append(total)
        out_grad = input_grad
    ordered = input_list[::-1]
    scale = (MICRO * BATCH * SEQ) ** (-0.5)
    stacked = [jnp.stack(target[::-1]) * scale for target in grad_lists]
    input_all = jnp.stack(ordered).reshape(LAYERS, MICRO, BATCH, SEQ, D)
    return (input_all, stacked[0], stacked[1], stacked[2], stacked[3])
```

```python
import functools

import jax
import jax.numpy as jnp
from jax import lax
from jax.experimental import pallas as pl
from jax.experimental.pallas import tpu as pltpu
from jax.sharding import PartitionSpec as P

HEAD_DIM = 128
SKEW = 2
CHUNK = 256
WIDE = 512
GROUP = 4

adapter_scale = 2.0
norm_eps = 1e-05

NT = (((1,), (1,)), ((), ()))
NN = (((1,), (0,)), ((), ()))
TN = (((0,), (0,)), ((), ()))


def dot(a, b, dims):
    return lax.dot_general(a, b, dims, preferred_element_type=jnp.float32)


def prep_body(
    w, q, k, v, hid, seed, att, alt, gain, upt, down, normed, lnq, lnv,
    wt, st, ato, alo, gno, upo, dno, ob, qb, vb, lb, normed_out, lnq_out, lnv_out,
    stage, wsems, sems,
):
    features = w.shape[0]
    columns = w.shape[1]
    depth = stage.shape[0]
    count = features // CHUNK
    micro = q.shape[0]
    loads = [
        pltpu.make_async_copy(src, st.at[pl.ds(i * micro, micro)], sems.at[i])
        for i, src in enumerate((q, k, v, hid, seed))
    ]
    pairs = ((att, ato), (alt, alo), (gain, gno), (upt, upo), (down, dno))
    loads += [pltpu.make_async_copy(s, d, sems.at[5 + i]) for i, (s, d) in enumerate(pairs)]

    def fetch(i, slot):
        rows = pl.ds(pl.multiple_of(i * CHUNK, CHUNK), CHUNK)
        return pltpu.make_async_copy(w.at[rows, :], stage.at[slot], wsems.at[slot])

    for i in range(depth - 1):
        fetch(i, i).start()
    for c in loads:
        c.start()

    def turn(i, carry):
        slot = lax.rem(i, depth)

        @pl.when(i + depth - 1 < count)
        def _():
            fetch(i + depth - 1, lax.rem(i + depth - 1, depth)).start()

        fetch(i, slot).wait()
        rows = pl.ds(pl.multiple_of(i * CHUNK, CHUNK), CHUNK)

        def block(j, inner):
            part = pl.ds(pl.multiple_of(j * CHUNK, CHUNK), CHUNK)
            wt[part, rows] = stage[slot, :, part].T
            return inner

        return lax.fori_loop(0, columns // CHUNK, block, carry, unroll=4)

    lax.fori_loop(0, count, turn, 0)
    for c in loads:
        c.wait()


def prep(w, q, k, v, hid, seed, att, alt, gain, upt, down, normed, lnq, lnv):
    any_spec = pl.BlockSpec(memory_space=pl.ANY)
    hbm = pl.BlockSpec(memory_space=pltpu.HBM)
    vmem = pl.BlockSpec(memory_space=pltpu.VMEM)
    bf = jnp.bfloat16
    outs = [
        pltpu.VMEM(w.shape[::-1], bf),
        pltpu.VMEM((5 * q.shape[0],) + q.shape[1:], bf),
    ] + [pltpu.VMEM(a.shape, a.dtype) for a in (att, alt, gain, upt, down)]
    rank2 = down.shape[0]
    outs += [jax.ShapeDtypeStruct(q.shape, bf)] * 3
    outs += [jax.ShapeDtypeStruct(q.shape[:2] + (rank2,), bf)]
    outs += [jax.ShapeDtypeStruct(a.shape, a.dtype) for a in (normed, lnq, lnv)]
    outs = pl.pallas_call(
        prep_body,
        out_shape=tuple(outs),
        in_specs=[hbm] * 14,
        out_specs=(vmem,) * 7 + (any_spec,) * 4 + (hbm,) * 3,
        input_output_aliases={11: 11, 12: 12, 13: 13},
        scratch_shapes=[
            pltpu.VMEM((3, CHUNK, w.shape[1]), bf),
            pltpu.SemaphoreType.DMA((3,)),
            pltpu.SemaphoreType.DMA((10,)),
        ],
        cost_estimate=pl.CostEstimate(flops=10**10, bytes_accessed=4 * w.size, transcendentals=0),
        compiler_params=pltpu.CompilerParams(vmem_limit_bytes=12 * 1024 * 1024),
        name="prep",
    )(*(
        pltpu.with_memory_space_constraint(a, pltpu.HBM)
        for a in (w, q, k, v, hid, seed, att, alt, gain, upt, down, normed, lnq, lnv)
    ))
    return outs[:7], outs[7:11], outs[11:]


def step_body(t, count, micro, *refs):
    x, refs = (refs[0], refs[1:]) if t >= SKEW else (None, refs)
    wt, st, att, alt, gain, upt, down = refs[:7]
    y, ob, qb, vb, lb = refs[18:23]
    xs, grads, scaled, lows, ys, sems = refs[23:]
    rows, features = xs.shape
    heads = features // HEAD_DIM
    scale = HEAD_DIM ** (-0.5)
    section = lax.axis_index("section")
    m = t - SKEW * (count - 1 - section)

    @pl.when(jnp.logical_and(m >= 0, m < micro))
    def _():
        if x is None:
            xs[...] = st[4 * micro + m]
        else:
            @pl.when(section == count - 1)
            def _():
                xs[...] = st[4 * micro + m]

            @pl.when(section != count - 1)
            def _():
                copy = pltpu.make_async_copy(x.at[0], xs, sems.at[0])
                copy.start()
                copy.wait()

        def some(i, carry):
            for u in range(GROUP):
                h = i * GROUP + u
                start = pl.multiple_of(h * HEAD_DIM, HEAD_DIM)
                f = pl.ds(start, HEAD_DIM)
                g = xs[:, f]
                a = att[m, h]
                ag = dot(g, st[2 * micro + m, :, f], NT)
                vg = dot(alt[m, h], g, NN).astype(jnp.bfloat16)
                total = jnp.sum(a * ag, axis=-1, keepdims=True)
                s = (a * (ag - total) * scale).astype(jnp.bfloat16)
                qg = dot(s, st[micro + m, :, f], NN).astype(jnp.bfloat16)
                kg = dot(s, st[m, :, f], TN).astype(jnp.bfloat16)
                grads[:, f] = qg
                grads[:, pl.ds(features + start, HEAD_DIM)] = vg
                grads[:, pl.ds(2 * features + start, HEAD_DIM)] = kg
            return carry

        lax.fori_loop(0, heads // GROUP, some, 0)
        low = (adapter_scale * dot(grads[:, : 2 * features], upt[...], NN)).astype(jnp.bfloat16)
        lows[...] = low
        saves = [
            pltpu.make_async_copy(grads.at[:, pl.ds(0, features)], qb.at[m], sems.at[1]),
            pltpu.make_async_copy(grads.at[:, pl.ds(features, features)], vb.at[m], sems.at[2]),
            pltpu.make_async_copy(lows, lb.at[m], sems.at[3]),
        ]
        for c in saves:
            c.start()

        def product(n, carry):
            part = pl.ds(pl.multiple_of(n * WIDE, WIDE), WIDE)
            ng = dot(grads[...], wt[:, part], NN) + dot(lows[...], down[:, part], NN)
            sc = gain[:, part] * ng
            scaled[:, part] = sc
            hf = st[3 * micro + m, :, part].astype(jnp.float32)
            corr, square = carry
            return (
                corr + jnp.sum(hf * sc, axis=-1, keepdims=True),
                square + jnp.sum(hf * hf, axis=-1, keepdims=True),
            )

        zero = jnp.zeros((rows, 1), jnp.float32)
        corr, square = lax.fori_loop(0, features // WIDE, product, (zero, zero))
        inverse = lax.rsqrt(square / features + norm_eps)
        corr = inverse**3 * (corr / features)
        ys[...] = (
            xs[...].astype(jnp.float32)
            + inverse * scaled[...]
            - st[3 * micro + m].astype(jnp.float32) * corr
        ).astype(jnp.bfloat16)
        sends = [
            pltpu.make_async_copy(ys, y.at[0], sems.at[4]),
            pltpu.make_async_copy(ys, ob.at[m], sems.at[5]),
        ]
        for c in sends:
            c.start()
        for c in saves + sends:
            c.wait()


def step(t, count, micro, x, held, buffers):
    wide, features = held[0].shape
    rows = held[1].shape[1]
    any_spec = pl.BlockSpec(memory_space=pl.ANY)
    vmem = pl.BlockSpec(memory_space=pltpu.VMEM)
    bf = jnp.bfloat16
    tile = pltpu.VMEM((rows, features), bf)
    out_shape = (
        tuple(pltpu.VMEM(a.shape, a.dtype) for a in held)
        + (jax.ShapeDtypeStruct((1, rows, features), bf),)
        + tuple(jax.ShapeDtypeStruct(b.shape, b.dtype) for b in buffers)
    )
    first = () if x is None else (x,)
    n = len(first)
    outs = pl.pallas_call(
        functools.partial(step_body, t, count, micro),
        out_shape=out_shape,
        in_specs=[any_spec] * n + [vmem] * 7 + [any_spec] * 4,
        out_specs=(vmem,) * 7 + (any_spec,) * 5,
        scratch_shapes=[
            tile,
            pltpu.VMEM((rows, wide), bf),
            pltpu.VMEM((rows, features), jnp.float32),
            pltpu.VMEM((rows, buffers[3].shape[2]), bf),
            tile,
            pltpu.SemaphoreType.DMA((6,)),
        ],
        input_output_aliases={
            **{n + i: i for i in range(7)},
            **{n + 7 + i: 8 + i for i in range(4)},
        },
        cost_estimate=pl.CostEstimate(
            flops=2 * rows * features * (wide + 4 * rows),
            bytes_accessed=4 * rows * features,
            transcendentals=0,
        ),
        compiler_params=pltpu.CompilerParams(vmem_limit_bytes=12 * 1024 * 1024),
        name="slot",
    )(*first, *held, *buffers)
    return outs[:7], outs[7], outs[8:]


def adapter_body(normed, lnq, lnv, qb, vb, lb, out):
    low = lb[...]
    rank = lnq.shape[1]
    out[: 2 * rank, :] = dot(low, normed[...], TN).astype(jnp.bfloat16)
    out[2 * rank : 3 * rank, :] = (adapter_scale * dot(lnq[...], qb[...], TN)).astype(jnp.bfloat16)
    out[3 * rank :, :] = (adapter_scale * dot(lnv[...], vb[...], TN)).astype(jnp.bfloat16)


def adapter(normed, lnq, lnv, qb, vb, lb):
    rank = lnq.shape[1]
    return pl.pallas_call(
        adapter_body,
        out_shape=jax.ShapeDtypeStruct((4 * rank, normed.shape[1]), jnp.bfloat16),
        cost_estimate=pl.CostEstimate(
            flops=8 * rank * normed.size, bytes_accessed=6 * normed.size, transcendentals=0
        ),
        name="adapter",
    )(normed, lnq, lnv, qb, vb, lb)


def on_device(
    hidden_in, queries, keys, values, cotangent, norm_gain, w_query, w_key, w_value,
    down_q, up_q, down_v, up_v,
):
    count = lax.axis_size("section")
    bf = jnp.bfloat16
    local = jnp.concatenate((w_query[0], w_value[0], w_key[0]), axis=1)
    w = lax.all_gather(local, "dp", axis=0, tiled=True)

    hid, q, k, v = hidden_in[0, :, 0], queries[0, :, 0], keys[0, :, 0], values[0, :, 0]
    seed = cotangent[:, 0]
    micro, positions, features = seed.shape
    rank = down_q.shape[1]
    heads = features // HEAD_DIM
    gain = norm_gain
    floated = hid.astype(jnp.float32)
    inverse = lax.rsqrt(jnp.mean(floated * floated, axis=-1, keepdims=True) + norm_eps)
    normed = (floated * inverse * gain).astype(bf).reshape(micro * positions, features)
    lnq = dot(normed, down_q[0], NT).astype(bf)
    lnv = dot(normed, down_v[0], NT).astype(bf)
    split = (micro, positions, heads, HEAD_DIM)
    scores = jnp.einsum(
        "nqhd,nkhd->nhqk", q.reshape(split), k.reshape(split), preferred_element_type=jnp.float32
    ) * (HEAD_DIM ** (-0.5))
    causal = lax.broadcasted_iota(jnp.int32, (positions, positions), 1) <= lax.broadcasted_iota(
        jnp.int32, (positions, positions), 0
    )
    att = jax.nn.softmax(jnp.where(causal, scores, -1e30), axis=-1)
    alt = att.astype(bf).transpose(0, 1, 3, 2)
    blank = jnp.zeros_like(up_q[0])
    upt = jnp.concatenate(
        (
            jnp.concatenate((up_q[0], blank), axis=1),
            jnp.concatenate((blank, up_v[0]), axis=1),
        ),
        axis=0,
    ).T
    down = jnp.concatenate((down_q[0], down_v[0]), axis=0)

    held, buffers, ready = prep(
        w, q, k, v, hid, seed, att, alt, gain, upt, down, normed, lnq, lnv
    )
    normed, lnq, lnv = ready
    incoming = {}
    slots = SKEW * (count - 1) + micro
    for t in range(slots):
        held, y, buffers = step(t, count, micro, incoming.get(t), held, buffers)
        pairs = [
            (s, s - 1)
            for s in range(1, count)
            if 0 <= t - SKEW * (count - 1 - s) < micro
        ]
        if pairs:
            incoming[t + SKEW] = lax.ppermute(y, "section", pairs)

    ob, qb, vb, lb = buffers
    flat = (micro * positions, features)
    sums = adapter(
        normed, lnq, lnv, qb.reshape(flat), vb.reshape(flat), lb.reshape(micro * positions, 2 * rank)
    )
    summed = lax.psum(sums, "dp").astype(jnp.float32)
    scale = (micro * positions * cotangent.shape[1] * lax.axis_size("dp")) ** (-0.5)
    summed = (summed * scale).reshape(4, 1, rank, features)
    return (ob[None, :, None], summed[0], summed[2], summed[1], summed[3])


def solution(mesh):
    placed = (
        P("section", None, "dp", None, None),
        P("section", None, "dp", None, None),
        P("section", None, "dp", None, None),
        P("section", None, "dp", None, None),
        P(None, "dp", None, None),
        P("section", None),
        P("section", "dp", None),
        P("section", "dp", None),
        P("section", "dp", None),
        P("section", None, None),
        P("section", None, None),
        P("section", None, None),
        P("section", None, None),
    )
    return jax.shard_map(
        on_device,
        mesh=mesh,
        in_specs=placed,
        out_specs=(
            P("section", None, "dp", None, None),
            P("section", None, None),
            P("section", None, None),
            P("section", None, None),
            P("section", None, None),
        ),
        check_vma=False,
    )
```

```python
import functools

import jax
import jax.numpy as jnp
from jax import lax
from jax.experimental import pallas as pl
from jax.experimental.pallas import tpu as pltpu
from jax.sharding import PartitionSpec as P

HEAD_DIM = 128
SKEW = 2
CHUNK = 256
WIDE = 512
GROUP = 4
DEPTH = 2048

adapter_scale = 2.0
norm_eps = 1e-05

NT = (((1,), (1,)), ((), ()))
NN = (((1,), (0,)), ((), ()))
TN = (((0,), (0,)), ((), ()))


def dot(a, b, dims):
    return lax.dot_general(a, b, dims, preferred_element_type=jnp.float32)


def prep_body(
    w, q, k, v, hid, seed, att, alt, gain, upt, down, normed, lnq, lnv,
    wt, st, ato, alo, gno, upo, dno, grads, lows, ob, normed_out, lnq_out, lnv_out,
    stage, wsems, sems,
):
    features = w.shape[0]
    columns = w.shape[1]
    depth = stage.shape[0]
    count = features // CHUNK
    micro = q.shape[0]
    loads = [
        pltpu.make_async_copy(src, st.at[pl.ds(i * micro, micro)], sems.at[i])
        for i, src in enumerate((q, k, v, hid, seed))
    ]
    pairs = ((att, ato), (alt, alo), (gain, gno), (upt, upo), (down, dno))
    loads += [pltpu.make_async_copy(s, d, sems.at[5 + i]) for i, (s, d) in enumerate(pairs)]

    def fetch(i, slot):
        rows = pl.ds(pl.multiple_of(i * CHUNK, CHUNK), CHUNK)
        return pltpu.make_async_copy(w.at[rows, :], stage.at[slot], wsems.at[slot])

    for i in range(depth - 1):
        fetch(i, i).start()
    for c in loads:
        c.start()

    def turn(i, carry):
        slot = lax.rem(i, depth)

        @pl.when(i + depth - 1 < count)
        def _():
            fetch(i + depth - 1, lax.rem(i + depth - 1, depth)).start()

        fetch(i, slot).wait()
        rows = pl.ds(pl.multiple_of(i * CHUNK, CHUNK), CHUNK)

        def block(j, inner):
            part = pl.ds(pl.multiple_of(j * CHUNK, CHUNK), CHUNK)
            wt[part, rows] = stage[slot, :, part].T
            return inner

        return lax.fori_loop(0, columns // CHUNK, block, carry, unroll=4)

    lax.fori_loop(0, count, turn, 0)
    for c in loads:
        c.wait()


def prep(w, q, k, v, hid, seed, att, alt, gain, upt, down, normed, lnq, lnv):
    hbm = pl.BlockSpec(memory_space=pltpu.HBM)
    vmem = pl.BlockSpec(memory_space=pltpu.VMEM)
    bf = jnp.bfloat16
    outs = [
        pltpu.VMEM(w.shape[::-1], bf),
        pltpu.VMEM((5 * q.shape[0],) + q.shape[1:], bf),
    ] + [pltpu.VMEM(a.shape, a.dtype) for a in (att, alt, gain, upt, down)]
    outs += [
        pltpu.VMEM(q.shape[:2] + (w.shape[1],), bf),
        pltpu.VMEM(q.shape[:2] + (down.shape[0],), bf),
        pltpu.VMEM(q.shape, bf),
    ]
    outs += [jax.ShapeDtypeStruct(a.shape, a.dtype) for a in (normed, lnq, lnv)]
    outs = pl.pallas_call(
        prep_body,
        out_shape=tuple(outs),
        in_specs=[hbm] * 14,
        out_specs=(vmem,) * 10 + (hbm,) * 3,
        input_output_aliases={11: 10, 12: 11, 13: 12},
        scratch_shapes=[
            pltpu.VMEM((2, CHUNK, w.shape[1]), bf),
            pltpu.SemaphoreType.DMA((2,)),
            pltpu.SemaphoreType.DMA((10,)),
        ],
        cost_estimate=pl.CostEstimate(flops=10**10, bytes_accessed=4 * w.size, transcendentals=0),
        compiler_params=pltpu.CompilerParams(vmem_limit_bytes=8 * 1024 * 1024),
        name="prep",
    )(*(
        pltpu.with_memory_space_constraint(a, pltpu.HBM)
        for a in (w, q, k, v, hid, seed, att, alt, gain, upt, down, normed, lnq, lnv)
    ))
    return outs[:10], outs[10:]


def step_body(t, count, micro, *refs):
    x, refs = (refs[0], refs[1:]) if t >= SKEW else (None, refs)
    wt, st, att, alt, gain, upt, down, grads, lows, ob = refs[:10]
    y = refs[20]
    xs, mids, lefts, scaled = refs[21:]
    rows, features = xs.shape
    heads = features // HEAD_DIM
    scale = HEAD_DIM ** (-0.5)
    section = lax.axis_index("section")
    m = t - SKEW * (count - 1 - section)

    @pl.when(jnp.logical_and(m >= 0, m < micro))
    def _():
        if x is None:
            xs[...] = st[4 * micro + m]
        elif t < micro:
            @pl.when(section == count - 1)
            def _():
                xs[...] = st[4 * micro + m]

            @pl.when(section != count - 1)
            def _():
                xs[...] = x[0]

        def given(f):
            return x[0, :, f] if t >= micro else xs[:, f]

        def each(body):
            def some(i, carry):
                for u in range(GROUP):
                    h = i * GROUP + u
                    body(h, pl.multiple_of(h * HEAD_DIM, HEAD_DIM))
                return carry

            lax.fori_loop(0, heads // GROUP, some, 0)

        def first(h, start):
            f = pl.ds(start, HEAD_DIM)
            g = given(f)
            mids[h] = dot(g, st[2 * micro + m, :, f], NT)
            vg = dot(alt[m, h], g, NN).astype(jnp.bfloat16)
            grads[m, :, pl.ds(features + start, HEAD_DIM)] = vg

        def second(h, start):
            a = att[m, h]
            ag = mids[h]
            total = jnp.sum(a * ag, axis=-1, keepdims=True)
            lefts[h] = (a * (ag - total) * scale).astype(jnp.bfloat16)

        def third(h, start):
            f = pl.ds(start, HEAD_DIM)
            s = lefts[h]
            grads[m, :, f] = dot(s, st[micro + m, :, f], NN).astype(jnp.bfloat16)
            kg = dot(s, st[m, :, f], TN).astype(jnp.bfloat16)
            grads[m, :, pl.ds(2 * features + start, HEAD_DIM)] = kg

        each(first)
        each(second)
        each(third)
        def over(width, right):
            return sum(
                dot(grads[m, :, k : k + DEPTH], right(pl.ds(k, DEPTH)), NN)
                for k in range(0, width, DEPTH)
            )

        low = adapter_scale * over(2 * features, lambda k: upt[k, :])
        lows[m] = low.astype(jnp.bfloat16)

        def product(n, carry):
            part = pl.ds(pl.multiple_of(n * WIDE, WIDE), WIDE)
            ng = over(3 * features, lambda k: wt[k, part]) + dot(lows[m], down[:, part], NN)
            sc = gain[:, part] * ng
            scaled[:, part] = sc
            hf = st[3 * micro + m, :, part].astype(jnp.float32)
            corr, square = carry
            return (
                corr + jnp.sum(hf * sc, axis=-1, keepdims=True),
                square + jnp.sum(hf * hf, axis=-1, keepdims=True),
            )

        zero = jnp.zeros((rows, 1), jnp.float32)
        corr, square = lax.fori_loop(0, features // WIDE, product, (zero, zero))
        inverse = lax.rsqrt(square / features + norm_eps)
        corr = inverse**3 * (corr / features)

        def finish(n, carry):
            f = pl.ds(pl.multiple_of(n * CHUNK, CHUNK), CHUNK)
            out = (
                given(f).astype(jnp.float32)
                + inverse * scaled[:, f]
                - st[3 * micro + m, :, f].astype(jnp.float32) * corr
            ).astype(jnp.bfloat16)
            y[0, :, f] = out
            ob[m, :, f] = out
            return carry

        lax.fori_loop(0, features // CHUNK, finish, 0, unroll=2)


def step(t, count, micro, x, held):
    wide, features = held[0].shape
    rows = held[1].shape[1]
    heads = features // HEAD_DIM
    vmem = pl.BlockSpec(memory_space=pltpu.VMEM)
    bf = jnp.bfloat16
    first = () if x is None else (pltpu.with_memory_space_constraint(x, pltpu.VMEM),)
    n = len(first)
    outs = pl.pallas_call(
        functools.partial(step_body, t, count, micro),
        out_shape=tuple(pltpu.VMEM(a.shape, a.dtype) for a in held)
        + (pltpu.VMEM((1, rows, features), bf),),
        in_specs=[vmem] * (n + 10),
        out_specs=(vmem,) * 11,
        scratch_shapes=[
            pltpu.VMEM((rows, features), bf),
            pltpu.VMEM((heads, rows, rows), jnp.float32),
            pltpu.VMEM((heads, rows, rows), bf),
            pltpu.VMEM((rows, features), jnp.float32),
        ],
        input_output_aliases={n + i: i for i in range(10)},
        cost_estimate=pl.CostEstimate(
            flops=2 * rows * features * (wide + 4 * rows),
            bytes_accessed=4 * rows * features,
            transcendentals=0,
        ),
        compiler_params=pltpu.CompilerParams(vmem_limit_bytes=8 * 1024 * 1024),
        name="slot",
    )(*first, *held)
    return outs[:10], outs[10]


def adapter_body(normed, lnq, lnv, grads, lows, ob, out, placed, sem):
    micro, rows, wide = grads.shape
    rank = lnq.shape[1]
    features = normed.shape[1]
    pieces = features // CHUNK
    copy = pltpu.make_async_copy(ob, placed, sem.at[0])
    copy.start()

    def piece(n, carry):
        start = pl.multiple_of(n * CHUNK, CHUNK)
        low = up_q = up_v = 0.0
        for m in range(micro):
            r = pl.ds(m * rows, rows)
            low += dot(lows[m], normed[r, pl.ds(start, CHUNK)], TN)
            up_q += dot(lnq[r, :], grads[m, :, pl.ds(start, CHUNK)], TN)
            up_v += dot(lnv[r, :], grads[m, :, pl.ds(features + start, CHUNK)], TN)
        out[n] = low[:rank].astype(jnp.bfloat16)
        out[pieces + n] = low[rank:].astype(jnp.bfloat16)
        out[2 * pieces + n] = (adapter_scale * up_q).astype(jnp.bfloat16)
        out[3 * pieces + n] = (adapter_scale * up_v).astype(jnp.bfloat16)
        return carry

    lax.fori_loop(0, pieces, piece, 0)
    copy.wait()


def adapter(normed, lnq, lnv, grads, lows, ob):
    rank = lnq.shape[1]
    pieces = normed.shape[1] // CHUNK
    vmem = pl.BlockSpec(memory_space=pltpu.VMEM)
    return pl.pallas_call(
        adapter_body,
        out_shape=(
            jax.ShapeDtypeStruct((4 * pieces, rank, CHUNK), jnp.bfloat16),
            jax.ShapeDtypeStruct(ob.shape, ob.dtype),
        ),
        in_specs=[vmem] * 6,
        out_specs=(vmem, pl.BlockSpec(memory_space=pltpu.HBM)),
        scratch_shapes=[pltpu.SemaphoreType.DMA((1,))],
        cost_estimate=pl.CostEstimate(
            flops=8 * rank * normed.size, bytes_accessed=6 * normed.size, transcendentals=0
        ),
        compiler_params=pltpu.CompilerParams(vmem_limit_bytes=8 * 1024 * 1024),
        name="adapter",
    )(normed, lnq, lnv, grads, lows, ob)


def summed_over(pieces, axis):
    devices = lax.axis_size(axis)
    split = (devices, pieces.shape[0] // devices) + pieces.shape[1:]
    parts = lax.all_to_all(pieces, axis, 0, 0, tiled=True).reshape(split)
    total = jnp.sum(parts.astype(jnp.float32), axis=0).astype(jnp.bfloat16)
    everyone = jnp.broadcast_to(total[None], split).reshape(pieces.shape)
    return lax.all_to_all(everyone, axis, 0, 0, tiled=True).astype(jnp.float32)


def on_device(
    hidden_in, queries, keys, values, cotangent, norm_gain, w_query, w_key, w_value,
    down_q, up_q, down_v, up_v,
):
    count = lax.axis_size("section")
    bf = jnp.bfloat16
    local = jnp.concatenate((w_query[0], w_value[0], w_key[0]), axis=1)
    w = lax.all_gather(local, "dp", axis=0, tiled=True)

    hid, q, k, v = hidden_in[0, :, 0], queries[0, :, 0], keys[0, :, 0], values[0, :, 0]
    seed = cotangent[:, 0]
    micro, positions, features = seed.shape
    rank = down_q.shape[1]
    heads = features // HEAD_DIM
    gain = norm_gain
    floated = hid.astype(jnp.float32)
    inverse = lax.rsqrt(jnp.mean(floated * floated, axis=-1, keepdims=True) + norm_eps)
    normed = (floated * inverse * gain).astype(bf).reshape(micro * positions, features)
    lnq = dot(normed, down_q[0], NT).astype(bf)
    lnv = dot(normed, down_v[0], NT).astype(bf)
    split = (micro, positions, heads, HEAD_DIM)
    scores = jnp.einsum(
        "nqhd,nkhd->nhqk", q.reshape(split), k.reshape(split), preferred_element_type=jnp.float32
    ) * (HEAD_DIM ** (-0.5))
    causal = lax.broadcasted_iota(jnp.int32, (positions, positions), 1) <= lax.broadcasted_iota(
        jnp.int32, (positions, positions), 0
    )
    att = jax.nn.softmax(jnp.where(causal, scores, -1e30), axis=-1)
    alt = att.astype(bf).transpose(0, 1, 3, 2)
    blank = jnp.zeros_like(up_q[0])
    upt = jnp.concatenate(
        (
            jnp.concatenate((up_q[0], blank), axis=1),
            jnp.concatenate((blank, up_v[0]), axis=1),
        ),
        axis=0,
    ).T
    down = jnp.concatenate((down_q[0], down_v[0]), axis=0)

    held, ready = prep(
        w, q, k, v, hid, seed, att, alt, gain, upt, down, normed, lnq, lnv
    )
    normed, lnq, lnv = ready
    incoming = {}
    slots = SKEW * (count - 1) + micro
    for t in range(slots):
        held, y = step(t, count, micro, incoming.get(t), held)
        pairs = [
            (s, s - 1)
            for s in range(1, count)
            if 0 <= t - SKEW * (count - 1 - s) < micro
        ]
        if pairs:
            incoming[t + SKEW] = lax.ppermute(y, "section", pairs)

    pieces, ob = adapter(normed, lnq, lnv, *held[7:])
    scale = (micro * positions * cotangent.shape[1] * lax.axis_size("dp")) ** (-0.5)
    summed = summed_over(pieces, "dp") * scale
    summed = summed.reshape(4, features // CHUNK, rank, CHUNK).transpose(0, 2, 1, 3)
    summed = summed.reshape(4, 1, rank, features)
    return (ob[None, :, None], summed[0], summed[2], summed[1], summed[3])


def solution(mesh):
    placed = (
        P("section", None, "dp", None, None),
        P("section", None, "dp", None, None),
        P("section", None, "dp", None, None),
        P("section", None, "dp", None, None),
        P(None, "dp", None, None),
        P("section", None),
        P("section", "dp", None),
        P("section", "dp", None),
        P("section", "dp", None),
        P("section", None, None),
        P("section", None, None),
        P("section", None, None),
        P("section", None, None),
    )
    return jax.shard_map(
        on_device,
        mesh=mesh,
        in_specs=placed,
        out_specs=(
            P("section", None, "dp", None, None),
            P("section", None, None),
            P("section", None, None),
            P("section", None, None),
            P("section", None, None),
        ),
        check_vma=False,
    )
```

```python
import functools

import jax
import jax.numpy as jnp
from jax import lax
from jax.experimental import pallas as pl
from jax.experimental.pallas import tpu as pltpu
from jax.sharding import PartitionSpec as P

HEAD_DIM = 128
SKEW = 2
CHUNK = 256
WIDE = 512
GROUP = 8
CUT = 2560
DEPTH = 2048

adapter_scale = 2.0
norm_eps = 1e-05

NT = (((1,), (1,)), ((), ()))
NN = (((1,), (0,)), ((), ()))
TN = (((0,), (0,)), ((), ()))


def dot(a, b, dims):
    return lax.dot_general(a, b, dims, preferred_element_type=jnp.float32)


X_SIDE = 4
Z_SIDE = 8


def shifted(block, side, distance):
    pairs = []
    for x in range(X_SIDE):
        for z in range(Z_SIDE):
            to = (
                ((x + distance) % X_SIDE) * Z_SIDE + z
                if side == X_SIDE
                else x * Z_SIDE + (z + distance) % Z_SIDE
            )
            pairs.append((x * Z_SIDE + z, to))
    return lax.ppermute(block, "dp", pairs)


def both_ways(block, side):
    found = [block]
    down = up = block
    for _ in range(side // 2 - 1):
        down, up = shifted(down, side, 1), shifted(up, side, -1)
        found += [down, up]
    half = block.shape[0] // 2
    return found + [shifted(down[:half], side, 1), shifted(up[half:], side, -1)]


def orders(side):
    return [0] + [d for k in range(1, side // 2) for d in (-k, k)] + [side // 2]


def gathered(local, cut):
    rows = jnp.concatenate(both_ways(local[:, :cut], X_SIDE), axis=0)
    planes = jnp.concatenate(both_ways(local[:, cut:], Z_SIDE), axis=0)
    return both_ways(rows, Z_SIDE), both_ways(planes, X_SIDE)


def pieces_of(blocks, outer, inner):
    found = []
    for at, block in enumerate(blocks):
        last = at >= outer - 1
        distance = outer // 2 if last else orders(outer)[at]
        units = orders(inner)
        if last:
            half = inner // 2
            units = units[:half] if at == outer - 1 else units[half:]
        found += [(block, u, distance, d) for u, d in enumerate(units)]
    return found


def prep_body(cut, *refs):
    first, refs = refs[: Z_SIDE + 1], refs[Z_SIDE + 1 :]
    second, refs = refs[: X_SIDE + 1], refs[X_SIDE + 1 :]
    q, k, v, hid, seed, att, alt, gain, upt, down = refs[:10]
    wt, st, ato, alo, gno, upo, dno = refs[13:20]
    stage, wsems, sems = refs[26:]
    features = wt.shape[1]
    total = wt.shape[0]
    width = stage.shape[2]
    micro = q.shape[0]
    unit = features // (X_SIDE * Z_SIDE)
    me = lax.axis_index("dp")
    my_x, my_z = me // Z_SIDE, lax.rem(me, Z_SIDE)
    loads = [
        pltpu.make_async_copy(src, st.at[pl.ds(i * micro, micro)], sems.at[i])
        for i, src in enumerate((q, k, v, hid, seed))
    ]
    pairs = ((att, ato), (alt, alo), (gain, gno), (upt, upo), (down, dno))
    loads += [pltpu.make_async_copy(s, d, sems.at[5 + i]) for i, (s, d) in enumerate(pairs)]

    def copies(start, slot, units):
        found = []
        for at, (ref, u, dx, dz) in enumerate(units):
            x = lax.rem(my_x + dx + X_SIDE, X_SIDE)
            z = lax.rem(my_z + dz + Z_SIDE, Z_SIDE)
            row = pl.multiple_of((x * Z_SIDE + z) * unit, unit)
            found.append(
                pltpu.make_async_copy(
                    ref.at[pl.ds(u * unit, unit), pl.ds(start, width)],
                    stage.at[slot, pl.ds(row, unit), :],
                    wsems.at[slot, at],
                )
            )
        return found

    by_x = [(r, u, dx, dz) for r, u, dz, dx in pieces_of(first, Z_SIDE, X_SIDE)]
    by_z = pieces_of(second, X_SIDE, Z_SIDE)

    def run(units, columns, base):
        count = columns // width

        def start(i, slot):
            for c in copies(pl.multiple_of(i * width, width), slot, units):
                c.start()

        start(0, 0)

        def turn(i, carry):
            slot = lax.rem(i, 2)

            @pl.when(i + 1 < count)
            def _():
                start(i + 1, 1 - slot)

            for c in copies(pl.multiple_of(i * width, width), slot, units):
                c.wait()

            def block(j, inner):
                rows = pl.ds(pl.multiple_of(j * CHUNK, CHUNK), CHUNK)
                to = pl.ds(pl.multiple_of(base + i * width, width), width)
                wt[to, rows] = stage[slot, rows, :].T
                return inner

            return lax.fori_loop(0, features // CHUNK, block, carry, unroll=2)

        lax.fori_loop(0, count, turn, 0)

    for c in loads:
        c.start()
    run(by_z, total - cut, cut)
    run(by_x, cut, 0)
    for c in loads:
        c.wait()


def prep(blocks, cut, q, k, v, hid, seed, att, alt, gain, upt, down, normed, lnq, lnv):
    hbm = pl.BlockSpec(memory_space=pltpu.HBM)
    vmem = pl.BlockSpec(memory_space=pltpu.VMEM)
    bf = jnp.bfloat16
    micro, rows, features = q.shape
    wide = 3 * features
    outs = [
        pltpu.VMEM((wide, features), bf),
        pltpu.VMEM((5 * micro, rows, features), bf),
    ] + [pltpu.VMEM(a.shape, a.dtype) for a in (att, alt, gain, upt, down)]
    outs += [
        pltpu.VMEM((micro, rows, wide), bf),
        pltpu.VMEM((micro, rows, down.shape[0]), bf),
        pltpu.VMEM(q.shape, bf),
    ]
    outs += [jax.ShapeDtypeStruct(a.shape, a.dtype) for a in (normed, lnq, lnv)]
    n = len(blocks)
    outs = pl.pallas_call(
        functools.partial(prep_body, cut),
        out_shape=tuple(outs),
        in_specs=[hbm] * (n + 13),
        out_specs=(vmem,) * 10 + (hbm,) * 3,
        input_output_aliases={n + 10: 10, n + 11: 11, n + 12: 12},
        scratch_shapes=[
            pltpu.VMEM((2, features, 2 * CHUNK), bf),
            pltpu.SemaphoreType.DMA((2, X_SIDE * Z_SIDE)),
            pltpu.SemaphoreType.DMA((10,)),
        ],
        cost_estimate=pl.CostEstimate(
            flops=10**10, bytes_accessed=4 * wide * features, transcendentals=0
        ),
        compiler_params=pltpu.CompilerParams(vmem_limit_bytes=8 * 1024 * 1024),
        name="prep",
    )(*(
        pltpu.with_memory_space_constraint(a, pltpu.HBM)
        for a in (*blocks, q, k, v, hid, seed, att, alt, gain, upt, down, normed, lnq, lnv)
    ))
    return outs[:10], outs[10:]


def step_body(t, count, micro, *refs):
    x, refs = (refs[0], refs[1:]) if t >= SKEW else (None, refs)
    wt, st, att, alt, gain, upt, down, grads, lows, ob = refs[:10]
    y = refs[20]
    xs, mids, lefts, scaled = refs[21:]
    rows, features = xs.shape
    heads = features // HEAD_DIM
    scale = HEAD_DIM ** (-0.5)
    section = lax.axis_index("section")
    m = t - SKEW * (count - 1 - section)

    @pl.when(jnp.logical_and(m >= 0, m < micro))
    def _():
        if x is None:
            xs[...] = st[4 * micro + m]
        elif t < micro:
            @pl.when(section == count - 1)
            def _():
                xs[...] = st[4 * micro + m]

            @pl.when(section != count - 1)
            def _():
                xs[...] = x[0]

        def given(f):
            return x[0, :, f] if t >= micro else xs[:, f]

        def each(body):
            def some(i, carry):
                for u in range(GROUP):
                    h = i * GROUP + u
                    body(h, pl.multiple_of(h * HEAD_DIM, HEAD_DIM))
                return carry

            lax.fori_loop(0, heads // GROUP, some, 0)

        def first(h, start):
            f = pl.ds(start, HEAD_DIM)
            g = given(f)
            mids[h] = dot(g, st[2 * micro + m, :, f], NT)
            vg = dot(alt[m, h], g, NN).astype(jnp.bfloat16)
            grads[m, :, pl.ds(features + start, HEAD_DIM)] = vg

        def second(h, start):
            a = att[m, h]
            ag = mids[h]
            total = jnp.sum(a * ag, axis=-1, keepdims=True)
            lefts[h] = (a * (ag - total) * scale).astype(jnp.bfloat16)

        def third(h, start):
            f = pl.ds(start, HEAD_DIM)
            s = lefts[h]
            grads[m, :, f] = dot(s, st[micro + m, :, f], NN).astype(jnp.bfloat16)
            kg = dot(s, st[m, :, f], TN).astype(jnp.bfloat16)
            grads[m, :, pl.ds(2 * features + start, HEAD_DIM)] = kg

        each(first)
        each(second)
        each(third)
        def over(width, right):
            return sum(
                dot(grads[m, :, k : k + DEPTH], right(pl.ds(k, DEPTH)), NN)
                for k in range(0, width, DEPTH)
            )

        low = adapter_scale * over(2 * features, lambda k: upt[k, :])
        lows[m] = low.astype(jnp.bfloat16)

        def product(n, carry):
            part = pl.ds(pl.multiple_of(n * WIDE, WIDE), WIDE)
            ng = over(3 * features, lambda k: wt[k, part]) + dot(lows[m], down[:, part], NN)
            sc = gain[:, part] * ng
            scaled[:, part] = sc
            hf = st[3 * micro + m, :, part].astype(jnp.float32)
            corr, square = carry
            return (
                corr + jnp.sum(hf * sc, axis=-1, keepdims=True),
                square + jnp.sum(hf * hf, axis=-1, keepdims=True),
            )

        zero = jnp.zeros((rows, 1), jnp.float32)
        corr, square = lax.fori_loop(0, features // WIDE, product, (zero, zero))
        inverse = lax.rsqrt(square / features + norm_eps)
        corr = inverse**3 * (corr / features)

        def finish(n, carry):
            f = pl.ds(pl.multiple_of(n * CHUNK, CHUNK), CHUNK)
            out = (
                given(f).astype(jnp.float32)
                + inverse * scaled[:, f]
                - st[3 * micro + m, :, f].astype(jnp.float32) * corr
            ).astype(jnp.bfloat16)
            y[0, :, f] = out
            ob[m, :, f] = out
            return carry

        lax.fori_loop(0, features // CHUNK, finish, 0, unroll=2)


def step(t, count, micro, x, held):
    wide, features = held[0].shape
    rows = held[1].shape[1]
    heads = features // HEAD_DIM
    vmem = pl.BlockSpec(memory_space=pltpu.VMEM)
    bf = jnp.bfloat16
    first = () if x is None else (pltpu.with_memory_space_constraint(x, pltpu.VMEM),)
    n = len(first)
    outs = pl.pallas_call(
        functools.partial(step_body, t, count, micro),
        out_shape=tuple(pltpu.VMEM(a.shape, a.dtype) for a in held)
        + (pltpu.VMEM((1, rows, features), bf),),
        in_specs=[vmem] * (n + 10),
        out_specs=(vmem,) * 11,
        scratch_shapes=[
            pltpu.VMEM((rows, features), bf),
            pltpu.VMEM((heads, rows, rows), jnp.float32),
            pltpu.VMEM((heads, rows, rows), bf),
            pltpu.VMEM((rows, features), jnp.float32),
        ],
        input_output_aliases={n + i: i for i in range(10)},
        cost_estimate=pl.CostEstimate(
            flops=2 * rows * features * (wide + 4 * rows),
            bytes_accessed=4 * rows * features,
            transcendentals=0,
        ),
        compiler_params=pltpu.CompilerParams(vmem_limit_bytes=8 * 1024 * 1024),
        name="slot",
    )(*first, *held)
    return outs[:10], outs[10]


def adapter_body(normed, lnq, lnv, grads, lows, ob, out, placed, sem):
    micro, rows, wide = grads.shape
    rank = lnq.shape[1]
    features = normed.shape[1]
    pieces = features // CHUNK
    copy = pltpu.make_async_copy(ob, placed, sem.at[0])
    copy.start()

    def piece(n, carry):
        start = pl.multiple_of(n * CHUNK, CHUNK)
        low = up_q = up_v = 0.0
        for m in range(micro):
            r = pl.ds(m * rows, rows)
            low += dot(lows[m], normed[r, pl.ds(start, CHUNK)], TN)
            up_q += dot(lnq[r, :], grads[m, :, pl.ds(start, CHUNK)], TN)
            up_v += dot(lnv[r, :], grads[m, :, pl.ds(features + start, CHUNK)], TN)
        out[n] = low[:rank].astype(jnp.bfloat16)
        out[pieces + n] = low[rank:].astype(jnp.bfloat16)
        out[2 * pieces + n] = (adapter_scale * up_q).astype(jnp.bfloat16)
        out[3 * pieces + n] = (adapter_scale * up_v).astype(jnp.bfloat16)
        return carry

    lax.fori_loop(0, pieces, piece, 0)
    copy.wait()


def adapter(normed, lnq, lnv, grads, lows, ob):
    rank = lnq.shape[1]
    pieces = normed.shape[1] // CHUNK
    vmem = pl.BlockSpec(memory_space=pltpu.VMEM)
    return pl.pallas_call(
        adapter_body,
        out_shape=(
            jax.ShapeDtypeStruct((4 * pieces, rank, CHUNK), jnp.bfloat16),
            jax.ShapeDtypeStruct(ob.shape, ob.dtype),
        ),
        in_specs=[vmem] * 6,
        out_specs=(vmem, pl.BlockSpec(memory_space=pltpu.HBM)),
        scratch_shapes=[pltpu.SemaphoreType.DMA((1,))],
        cost_estimate=pl.CostEstimate(
            flops=8 * rank * normed.size, bytes_accessed=6 * normed.size, transcendentals=0
        ),
        compiler_params=pltpu.CompilerParams(vmem_limit_bytes=8 * 1024 * 1024),
        name="adapter",
    )(normed, lnq, lnv, grads, lows, ob)


def summed_over(pieces, axis):
    devices = lax.axis_size(axis)
    split = (devices, pieces.shape[0] // devices) + pieces.shape[1:]
    parts = lax.all_to_all(pieces, axis, 0, 0, tiled=True).reshape(split)
    total = jnp.sum(parts.astype(jnp.float32), axis=0).astype(jnp.bfloat16)
    everyone = jnp.broadcast_to(total[None], split).reshape(pieces.shape)
    return lax.all_to_all(everyone, axis, 0, 0, tiled=True).astype(jnp.float32)


def on_device(
    hidden_in, queries, keys, values, cotangent, norm_gain, w_query, w_key, w_value,
    down_q, up_q, down_v, up_v,
):
    count = lax.axis_size("section")
    bf = jnp.bfloat16
    local = jnp.concatenate((w_query[0], w_value[0], w_key[0]), axis=1)
    by_x, by_z = gathered(local, CUT)

    hid, q, k, v = hidden_in[0, :, 0], queries[0, :, 0], keys[0, :, 0], values[0, :, 0]
    seed = cotangent[:, 0]
    micro, positions, features = seed.shape
    rank = down_q.shape[1]
    heads = features // HEAD_DIM
    gain = norm_gain
    floated = hid.astype(jnp.float32)
    inverse = lax.rsqrt(jnp.mean(floated * floated, axis=-1, keepdims=True) + norm_eps)
    normed = (floated * inverse * gain).astype(bf).reshape(micro * positions, features)
    lnq = dot(normed, down_q[0], NT).astype(bf)
    lnv = dot(normed, down_v[0], NT).astype(bf)
    split = (micro, positions, heads, HEAD_DIM)
    scores = jnp.einsum(
        "nqhd,nkhd->nhqk", q.reshape(split), k.reshape(split), preferred_element_type=jnp.float32
    ) * (HEAD_DIM ** (-0.5))
    causal = lax.broadcasted_iota(jnp.int32, (positions, positions), 1) <= lax.broadcasted_iota(
        jnp.int32, (positions, positions), 0
    )
    att = jax.nn.softmax(jnp.where(causal, scores, -1e30), axis=-1)
    alt = att.astype(bf).transpose(0, 1, 3, 2)
    blank = jnp.zeros_like(up_q[0])
    upt = jnp.concatenate(
        (
            jnp.concatenate((up_q[0], blank), axis=1),
            jnp.concatenate((blank, up_v[0]), axis=1),
        ),
        axis=0,
    ).T
    down = jnp.concatenate((down_q[0], down_v[0]), axis=0)

    held, ready = prep(
        (*by_x, *by_z), CUT, q, k, v, hid, seed, att, alt, gain, upt, down, normed, lnq, lnv
    )
    normed, lnq, lnv = ready
    incoming = {}
    slots = SKEW * (count - 1) + micro
    for t in range(slots):
        held, y = step(t, count, micro, incoming.get(t), held)
        pairs = [
            (s, s - 1)
            for s in range(1, count)
            if 0 <= t - SKEW * (count - 1 - s) < micro
        ]
        if pairs:
            incoming[t + SKEW] = lax.ppermute(y, "section", pairs)

    pieces, ob = adapter(normed, lnq, lnv, *held[7:])
    scale = (micro * positions * cotangent.shape[1] * lax.axis_size("dp")) ** (-0.5)
    summed = summed_over(pieces, "dp") * scale
    summed = summed.reshape(4, features // CHUNK, rank, CHUNK).transpose(0, 2, 1, 3)
    summed = summed.reshape(4, 1, rank, features)
    return (ob[None, :, None], summed[0], summed[2], summed[1], summed[3])


def solution(mesh):
    placed = (
        P("section", None, "dp", None, None),
        P("section", None, "dp", None, None),
        P("section", None, "dp", None, None),
        P("section", None, "dp", None, None),
        P(None, "dp", None, None),
        P("section", None),
        P("section", "dp", None),
        P("section", "dp", None),
        P("section", "dp", None),
        P("section", None, None),
        P("section", None, None),
        P("section", None, None),
        P("section", None, None),
    )
    return jax.shard_map(
        on_device,
        mesh=mesh,
        in_specs=placed,
        out_specs=(
            P("section", None, "dp", None, None),
            P("section", None, None),
            P("section", None, None),
            P("section", None, None),
            P("section", None, None),
        ),
        check_vma=False,
    )
```

```python
import functools

import jax
import jax.numpy as jnp
from jax import lax
from jax.experimental import pallas as pl
from jax.experimental.pallas import tpu as pltpu
from jax.sharding import PartitionSpec as P

HEAD_DIM = 128
SKEW = 2
CHUNK = 256
WIDE = 512
GROUP = 8
CUT = 2560
DEPTH = 2048

adapter_scale = 2.0
norm_eps = 1e-05

NT = (((1,), (1,)), ((), ()))
NN = (((1,), (0,)), ((), ()))
TN = (((0,), (0,)), ((), ()))


def dot(a, b, dims):
    return lax.dot_general(a, b, dims, preferred_element_type=jnp.float32)


X_SIDE = 4
Z_SIDE = 8


def shifted(block, side, distance):
    pairs = []
    for x in range(X_SIDE):
        for z in range(Z_SIDE):
            to = (
                ((x + distance) % X_SIDE) * Z_SIDE + z
                if side == X_SIDE
                else x * Z_SIDE + (z + distance) % Z_SIDE
            )
            pairs.append((x * Z_SIDE + z, to))
    return lax.ppermute(block, "dp", pairs)


def both_ways(block, side):
    found = [block]
    down = up = block
    for _ in range(side // 2 - 1):
        down, up = shifted(down, side, 1), shifted(up, side, -1)
        found += [down, up]
    half = block.shape[0] // 2
    return found + [shifted(down[:half], side, 1), shifted(up[half:], side, -1)]


def orders(side):
    return [0] + [d for k in range(1, side // 2) for d in (-k, k)] + [side // 2]


def gathered(local, cut):
    planes = both_ways(local[:, cut:], Z_SIDE)
    top = jnp.concatenate(planes[: Z_SIDE // 2], axis=0)
    bottom = jnp.concatenate(planes[Z_SIDE // 2 :], axis=0)
    rows = jnp.concatenate(both_ways(local[:, :cut], X_SIDE), axis=0)
    top_down, top_up = shifted(top, X_SIDE, 1), shifted(top, X_SIDE, -1)
    rows, bottom, forward = lax.optimization_barrier((rows, bottom, top_down))
    low_down, low_up = shifted(bottom, X_SIDE, 1), shifted(bottom, X_SIDE, -1)
    tops = [top, top_down, top_up, shifted(forward, X_SIDE, 1)]
    bottoms = [bottom, low_down, low_up, shifted(low_up, X_SIDE, -1)]
    return both_ways(rows, Z_SIDE), tops + bottoms


def pieces_of(blocks, outer, inner):
    found = []
    for at, block in enumerate(blocks):
        last = at >= outer - 1
        distance = outer // 2 if last else orders(outer)[at]
        units = orders(inner)
        if last:
            half = inner // 2
            units = units[:half] if at == outer - 1 else units[half:]
        found += [(block, u, distance, d) for u, d in enumerate(units)]
    return found


def halves_of(blocks, outer, inner):
    half = inner // 2
    return [
        (block, u, orders(outer)[at % outer], orders(inner)[u + half * (at // outer)])
        for at, block in enumerate(blocks)
        for u in range(half)
    ]


def prep_body(cut, *refs):
    first, refs = refs[: Z_SIDE + 1], refs[Z_SIDE + 1 :]
    second, refs = refs[: 2 * X_SIDE], refs[2 * X_SIDE :]
    q, k, v, hid, seed, att, alt, gain, upt, down = refs[:10]
    wt, st, ato, alo, gno, upo, dno = refs[13:20]
    stage, wsems, sems = refs[26:]
    features = wt.shape[1]
    total = wt.shape[0]
    width = stage.shape[2]
    micro = q.shape[0]
    unit = features // (X_SIDE * Z_SIDE)
    me = lax.axis_index("dp")
    my_x, my_z = me // Z_SIDE, lax.rem(me, Z_SIDE)
    loads = [
        pltpu.make_async_copy(src, st.at[pl.ds(i * micro, micro)], sems.at[i])
        for i, src in enumerate((q, k, v, hid, seed))
    ]
    pairs = ((att, ato), (alt, alo), (gain, gno), (upt, upo), (down, dno))
    loads += [pltpu.make_async_copy(s, d, sems.at[5 + i]) for i, (s, d) in enumerate(pairs)]

    def copies(start, slot, units):
        found = []
        for at, (ref, u, dx, dz) in enumerate(units):
            x = lax.rem(my_x + dx + X_SIDE, X_SIDE)
            z = lax.rem(my_z + dz + Z_SIDE, Z_SIDE)
            row = pl.multiple_of((x * Z_SIDE + z) * unit, unit)
            found.append(
                pltpu.make_async_copy(
                    ref.at[pl.ds(u * unit, unit), pl.ds(start, width)],
                    stage.at[slot, pl.ds(row, unit), :],
                    wsems.at[slot, at],
                )
            )
        return found

    by_x = [(r, u, dx, dz) for r, u, dz, dx in pieces_of(first, Z_SIDE, X_SIDE)]
    by_z = halves_of(second, X_SIDE, Z_SIDE)

    def run(units, columns, base):
        count = columns // width

        def start(i, slot):
            for c in copies(pl.multiple_of(i * width, width), slot, units):
                c.start()

        start(0, 0)

        def turn(i, carry):
            slot = lax.rem(i, 2)

            @pl.when(i + 1 < count)
            def _():
                start(i + 1, 1 - slot)

            for c in copies(pl.multiple_of(i * width, width), slot, units):
                c.wait()

            def block(j, inner):
                rows = pl.ds(pl.multiple_of(j * CHUNK, CHUNK), CHUNK)
                to = pl.ds(pl.multiple_of(base + i * width, width), width)
                wt[to, rows] = stage[slot, rows, :].T
                return inner

            return lax.fori_loop(0, features // CHUNK, block, carry, unroll=4)

        lax.fori_loop(0, count, turn, 0)

    for c in loads:
        c.start()
    run(by_z, total - cut, cut)
    run(by_x, cut, 0)
    for c in loads:
        c.wait()


def prep(blocks, cut, q, k, v, hid, seed, att, alt, gain, upt, down, normed, lnq, lnv):
    hbm = pl.BlockSpec(memory_space=pltpu.HBM)
    vmem = pl.BlockSpec(memory_space=pltpu.VMEM)
    bf = jnp.bfloat16
    micro, rows, features = q.shape
    wide = 3 * features
    outs = [
        pltpu.VMEM((wide, features), bf),
        pltpu.VMEM((5 * micro, rows, features), bf),
    ] + [pltpu.VMEM(a.shape, a.dtype) for a in (att, alt, gain, upt, down)]
    outs += [
        pltpu.VMEM((micro, rows, wide), bf),
        pltpu.VMEM((micro, rows, down.shape[0]), bf),
        pltpu.VMEM(q.shape, bf),
    ]
    outs += [jax.ShapeDtypeStruct(a.shape, a.dtype) for a in (normed, lnq, lnv)]
    n = len(blocks)
    outs = pl.pallas_call(
        functools.partial(prep_body, cut),
        out_shape=tuple(outs),
        in_specs=[hbm] * (n + 13),
        out_specs=(vmem,) * 10 + (hbm,) * 3,
        input_output_aliases={n + 10: 10, n + 11: 11, n + 12: 12},
        scratch_shapes=[
            pltpu.VMEM((2, features, 2 * CHUNK), bf),
            pltpu.SemaphoreType.DMA((2, X_SIDE * Z_SIDE)),
            pltpu.SemaphoreType.DMA((10,)),
        ],
        cost_estimate=pl.CostEstimate(
            flops=10**10, bytes_accessed=4 * wide * features, transcendentals=0
        ),
        compiler_params=pltpu.CompilerParams(vmem_limit_bytes=8 * 1024 * 1024),
        name="prep",
    )(*(
        pltpu.with_memory_space_constraint(a, pltpu.HBM)
        for a in (*blocks, q, k, v, hid, seed, att, alt, gain, upt, down, normed, lnq, lnv)
    ))
    return outs[:10], outs[10:]


def step_body(t, count, micro, *refs):
    x, refs = (refs[0], refs[1:]) if t >= SKEW else (None, refs)
    wt, st, att, alt, gain, upt, down, grads, lows, ob = refs[:10]
    y = refs[20]
    xs, mids, lefts, scaled = refs[21:]
    rows, features = xs.shape
    heads = features // HEAD_DIM
    scale = HEAD_DIM ** (-0.5)
    section = lax.axis_index("section")
    m = t - SKEW * (count - 1 - section)

    @pl.when(jnp.logical_and(m >= 0, m < micro))
    def _():
        if x is None:
            xs[...] = st[4 * micro + m]
        elif t < micro:
            @pl.when(section == count - 1)
            def _():
                xs[...] = st[4 * micro + m]

            @pl.when(section != count - 1)
            def _():
                xs[...] = x[0]

        def given(f):
            return x[0, :, f] if t >= micro else xs[:, f]

        def each(body):
            def some(i, carry):
                for u in range(GROUP):
                    h = i * GROUP + u
                    body(h, pl.multiple_of(h * HEAD_DIM, HEAD_DIM))
                return carry

            lax.fori_loop(0, heads // GROUP, some, 0)

        def first(h, start):
            f = pl.ds(start, HEAD_DIM)
            g = given(f)
            mids[h] = dot(g, st[2 * micro + m, :, f], NT)
            vg = dot(alt[m, h], g, NN).astype(jnp.bfloat16)
            grads[m, :, pl.ds(features + start, HEAD_DIM)] = vg

        def second(h, start):
            a = att[m, h]
            ag = mids[h]
            total = jnp.sum(a * ag, axis=-1, keepdims=True)
            lefts[h] = (a * (ag - total) * scale).astype(jnp.bfloat16)

        def third(h, start):
            f = pl.ds(start, HEAD_DIM)
            s = lefts[h]
            grads[m, :, f] = dot(s, st[micro + m, :, f], NN).astype(jnp.bfloat16)
            kg = dot(s, st[m, :, f], TN).astype(jnp.bfloat16)
            grads[m, :, pl.ds(2 * features + start, HEAD_DIM)] = kg

        each(first)
        each(second)
        each(third)
        def over(width, right):
            return sum(
                dot(grads[m, :, k : k + DEPTH], right(pl.ds(k, DEPTH)), NN)
                for k in range(0, width, DEPTH)
            )

        low = adapter_scale * over(2 * features, lambda k: upt[k, :])
        lows[m] = low.astype(jnp.bfloat16)

        def product(n, carry):
            part = pl.ds(pl.multiple_of(n * WIDE, WIDE), WIDE)
            ng = over(3 * features, lambda k: wt[k, part]) + dot(lows[m], down[:, part], NN)
            sc = gain[:, part] * ng
            scaled[:, part] = sc
            hf = st[3 * micro + m, :, part].astype(jnp.float32)
            corr, square = carry
            return (
                corr + jnp.sum(hf * sc, axis=-1, keepdims=True),
                square + jnp.sum(hf * hf, axis=-1, keepdims=True),
            )

        zero = jnp.zeros((rows, 1), jnp.float32)
        corr, square = lax.fori_loop(0, features // WIDE, product, (zero, zero))
        inverse = lax.rsqrt(square / features + norm_eps)
        corr = inverse**3 * (corr / features)

        def finish(n, carry):
            f = pl.ds(pl.multiple_of(n * CHUNK, CHUNK), CHUNK)
            out = (
                given(f).astype(jnp.float32)
                + inverse * scaled[:, f]
                - st[3 * micro + m, :, f].astype(jnp.float32) * corr
            ).astype(jnp.bfloat16)
            y[0, :, f] = out
            ob[m, :, f] = out
            return carry

        lax.fori_loop(0, features // CHUNK, finish, 0, unroll=2)


def step(t, count, micro, x, held):
    wide, features = held[0].shape
    rows = held[1].shape[1]
    heads = features // HEAD_DIM
    vmem = pl.BlockSpec(memory_space=pltpu.VMEM)
    bf = jnp.bfloat16
    first = () if x is None else (pltpu.with_memory_space_constraint(x, pltpu.VMEM),)
    n = len(first)
    outs = pl.pallas_call(
        functools.partial(step_body, t, count, micro),
        out_shape=tuple(pltpu.VMEM(a.shape, a.dtype) for a in held)
        + (pltpu.VMEM((1, rows, features), bf),),
        in_specs=[vmem] * (n + 10),
        out_specs=(vmem,) * 11,
        scratch_shapes=[
            pltpu.VMEM((rows, features), bf),
            pltpu.VMEM((heads, rows, rows), jnp.float32),
            pltpu.VMEM((heads, rows, rows), bf),
            pltpu.VMEM((rows, features), jnp.float32),
        ],
        input_output_aliases={n + i: i for i in range(10)},
        cost_estimate=pl.CostEstimate(
            flops=2 * rows * features * (wide + 4 * rows),
            bytes_accessed=4 * rows * features,
            transcendentals=0,
        ),
        compiler_params=pltpu.CompilerParams(vmem_limit_bytes=8 * 1024 * 1024),
        name="slot",
    )(*first, *held)
    return outs[:10], outs[10]


def adapter_body(normed, lnq, lnv, grads, lows, ob, out, placed, sem):
    micro, rows, wide = grads.shape
    rank = lnq.shape[1]
    features = normed.shape[1]
    pieces = features // CHUNK
    copy = pltpu.make_async_copy(ob, placed, sem.at[0])
    copy.start()

    def piece(n, carry):
        start = pl.multiple_of(n * CHUNK, CHUNK)
        low = up_q = up_v = 0.0
        for m in range(micro):
            r = pl.ds(m * rows, rows)
            low += dot(lows[m], normed[r, pl.ds(start, CHUNK)], TN)
            up_q += dot(lnq[r, :], grads[m, :, pl.ds(start, CHUNK)], TN)
            up_v += dot(lnv[r, :], grads[m, :, pl.ds(features + start, CHUNK)], TN)
        out[n] = low[:rank].astype(jnp.bfloat16)
        out[pieces + n] = low[rank:].astype(jnp.bfloat16)
        out[2 * pieces + n] = (adapter_scale * up_q).astype(jnp.bfloat16)
        out[3 * pieces + n] = (adapter_scale * up_v).astype(jnp.bfloat16)
        return carry

    lax.fori_loop(0, pieces, piece, 0)
    copy.wait()


def adapter(normed, lnq, lnv, grads, lows, ob):
    rank = lnq.shape[1]
    pieces = normed.shape[1] // CHUNK
    vmem = pl.BlockSpec(memory_space=pltpu.VMEM)
    return pl.pallas_call(
        adapter_body,
        out_shape=(
            jax.ShapeDtypeStruct((4 * pieces, rank, CHUNK), jnp.bfloat16),
            jax.ShapeDtypeStruct(ob.shape, ob.dtype),
        ),
        in_specs=[vmem] * 6,
        out_specs=(vmem, pl.BlockSpec(memory_space=pltpu.HBM)),
        scratch_shapes=[pltpu.SemaphoreType.DMA((1,))],
        cost_estimate=pl.CostEstimate(
            flops=8 * rank * normed.size, bytes_accessed=6 * normed.size, transcendentals=0
        ),
        compiler_params=pltpu.CompilerParams(vmem_limit_bytes=8 * 1024 * 1024),
        name="adapter",
    )(normed, lnq, lnv, grads, lows, ob)


def summed_over(pieces, axis):
    devices = lax.axis_size(axis)
    split = (devices, pieces.shape[0] // devices) + pieces.shape[1:]
    parts = lax.all_to_all(pieces, axis, 0, 0, tiled=True).reshape(split)
    total = jnp.sum(parts.astype(jnp.float32), axis=0).astype(jnp.bfloat16)
    everyone = jnp.broadcast_to(total[None], split).reshape(pieces.shape)
    return lax.all_to_all(everyone, axis, 0, 0, tiled=True).astype(jnp.float32)


def on_device(
    hidden_in, queries, keys, values, cotangent, norm_gain, w_query, w_key, w_value,
    down_q, up_q, down_v, up_v,
):
    count = lax.axis_size("section")
    bf = jnp.bfloat16
    local = jnp.concatenate((w_query[0], w_value[0], w_key[0]), axis=1)
    by_x, by_z = gathered(local, CUT)

    hid, q, k, v = hidden_in[0, :, 0], queries[0, :, 0], keys[0, :, 0], values[0, :, 0]
    seed = cotangent[:, 0]
    micro, positions, features = seed.shape
    rank = down_q.shape[1]
    heads = features // HEAD_DIM
    gain = norm_gain
    floated = hid.astype(jnp.float32)
    inverse = lax.rsqrt(jnp.mean(floated * floated, axis=-1, keepdims=True) + norm_eps)
    normed = (floated * inverse * gain).astype(bf).reshape(micro * positions, features)
    lnq = dot(normed, down_q[0], NT).astype(bf)
    lnv = dot(normed, down_v[0], NT).astype(bf)
    split = (micro, positions, heads, HEAD_DIM)
    scores = jnp.einsum(
        "nqhd,nkhd->nhqk", q.reshape(split), k.reshape(split), preferred_element_type=jnp.float32
    ) * (HEAD_DIM ** (-0.5))
    causal = lax.broadcasted_iota(jnp.int32, (positions, positions), 1) <= lax.broadcasted_iota(
        jnp.int32, (positions, positions), 0
    )
    att = jax.nn.softmax(jnp.where(causal, scores, -1e30), axis=-1)
    alt = att.astype(bf).transpose(0, 1, 3, 2)
    blank = jnp.zeros_like(up_q[0])
    upt = jnp.concatenate(
        (
            jnp.concatenate((up_q[0], blank), axis=1),
            jnp.concatenate((blank, up_v[0]), axis=1),
        ),
        axis=0,
    ).T
    down = jnp.concatenate((down_q[0], down_v[0]), axis=0)

    held, ready = prep(
        (*by_x, *by_z), CUT, q, k, v, hid, seed, att, alt, gain, upt, down, normed, lnq, lnv
    )
    normed, lnq, lnv = ready
    incoming = {}
    slots = SKEW * (count - 1) + micro
    for t in range(slots):
        held, y = step(t, count, micro, incoming.get(t), held)
        pairs = [
            (s, s - 1)
            for s in range(1, count)
            if 0 <= t - SKEW * (count - 1 - s) < micro
        ]
        if pairs:
            incoming[t + SKEW] = lax.ppermute(y, "section", pairs)

    pieces, ob = adapter(normed, lnq, lnv, *held[7:])
    scale = (micro * positions * cotangent.shape[1] * lax.axis_size("dp")) ** (-0.5)
    summed = summed_over(pieces, "dp") * scale
    summed = summed.reshape(4, features // CHUNK, rank, CHUNK).transpose(0, 2, 1, 3)
    summed = summed.reshape(4, 1, rank, features)
    return (ob[None, :, None], summed[0], summed[2], summed[1], summed[3])


def solution(mesh):
    placed = (
        P("section", None, "dp", None, None),
        P("section", None, "dp", None, None),
        P("section", None, "dp", None, None),
        P("section", None, "dp", None, None),
        P(None, "dp", None, None),
        P("section", None),
        P("section", "dp", None),
        P("section", "dp", None),
        P("section", "dp", None),
        P("section", None, None),
        P("section", None, None),
        P("section", None, None),
        P("section", None, None),
    )
    return jax.shard_map(
        on_device,
        mesh=mesh,
        in_specs=placed,
        out_specs=(
            P("section", None, "dp", None, None),
            P("section", None, None),
            P("section", None, None),
            P("section", None, None),
            P("section", None, None),
        ),
        check_vma=False,
    )
```
